32 devices in a mesh: dp: 8 (over z, y), mp: 4 (over x, core).
Axes of the slice: x: 2, y: 2, z: 4, core: 2. Of those that a mesh axis runs over, the one named last changes fastest.
Arguments:
- clean: bfloat16 [16, 128, 2432], P('dp'), may hold values from -6 to 6
- noise: bfloat16 [16, 128, 2432], P('dp'), may hold values from -6 to 6
- modulation: float32 [16, 7296], P('dp'), may hold values from -3 to 3
- strata: int32 [16], P('dp'), may hold values from 0 to 63
- up_weight: bfloat16 [2432, 5376], P(None, 'mp'), may hold values from -0.125 to 0.125
- down_weight: bfloat16 [5376, 2432], P('mp'), may hold values from -0.078125 to 0.078125
Outputs:
- up_gradient: float32 [5376, 2432], P(('mp', 'dp'))
- loss_value: float32 [], replicated
The draws below stay inside these ranges and needn't reach their ends.
All inputs are finite; a program needn't handle non-finite values.
Results may differ from the reference program's by a relative error of at most 0.008.
Values may be sent and summed in bfloat16 or wider, within the bound.
A program may use at most 128 MiB of HBM per device.

```python
import math
import jax
import jax.numpy as jnp
from jax import lax

D = 2432
FFW = 5376
ROWS = 128
STRATA = 64
SAMPLES = 16
N_MP = 4


def draw_strata(key, part):
    middle = STRATA // 2
    positions = jnp.arange(SAMPLES, dtype=jnp.int32)
    base_dist = (SAMPLES - 1 - positions) * (middle - 3) // SAMPLES
    jitter = jax.random.randint(jax.random.fold_in(key, 11), (SAMPLES,), 0, 3, dtype=jnp.int32)
    distance = jnp.minimum(base_dist + jitter, middle - 1)
    side_bit = jax.random.randint(jax.random.fold_in(key, 12), (SAMPLES,), 0, 2, dtype=jnp.int32)
    upper = middle + distance
    lower = middle - 1 - distance
    return jnp.where(side_bit == 1, upper, lower).astype(jnp.int32)


def level_of(key, dims, pieces, smallest, top_value):
    loudness, own = 1.0, jax.random.fold_in(key, 6)
    for position, parts in pieces:
        heights = jnp.exp(jax.random.uniform(jax.random.fold_in(own, position), (parts,), jnp.float32, smallest / len(pieces), top_value / len(pieces)))
        loudness = loudness * jnp.repeat(heights, dims[position] // parts).reshape([-1 if axis == position else 1 for axis in range(len(dims))])
    return loudness


def scatter_about(own_key, extent, deviation, most, shards=(), held_as=jnp.bfloat16):
    factor_of = level_of(own_key, extent, shards, -0.22, 0.18) if shards else 1.0
    array = jax.random.normal(own_key, extent, jnp.float32) * deviation * factor_of
    return jnp.minimum(jnp.maximum(array, -most), most).astype(held_as)


def setup_inputs(seed: int = 0) -> dict:
    splits = jax.random.split(jax.random.key(seed), 7)
    return {
        "clean": scatter_about(splits[0], (SAMPLES, ROWS, D), 1.0, 6.0, ((0, 8),)),
        "noise": scatter_about(splits[1], (SAMPLES, ROWS, D), 1.0, 6.0, ((0, 8),)),
        "modulation": scatter_about(splits[2], (SAMPLES, 3 * D), 0.5, 3.0, ((0, 8),), jnp.float32),
        "strata": draw_strata(jax.random.fold_in(splits[6], 71), 0),
        "up_weight": scatter_about(splits[4], (D, FFW), D ** -0.5, 0.125, ((1, 4),)),
        "down_weight": scatter_about(splits[5], (FFW, D), FFW ** -0.5, 0.078125, ((0, 4),)),
    }


loss_scale = 1048576.0

def stratum_weights(strata):
    quantile = (strata.astype(jnp.float32) + 0.5) / STRATA
    levels = math.sqrt(2.0) * lax.erf_inv(2.0 * quantile - 1.0)
    fraction = jax.nn.sigmoid(levels)
    weight = jnp.exp(-0.5 * levels * levels) / (math.sqrt(2.0 * math.pi) * fraction * (1.0 - fraction))
    return (fraction, weight)

def modulate(clean, noise, modulation, fraction):
    features = clean.shape[-1]
    anchor = clean.astype(jnp.float32)
    drift_field = noise.astype(jnp.float32)
    mix_frac = fraction[:, None, None]
    noisy_field = (1.0 - mix_frac) * anchor + mix_frac * drift_field
    target = drift_field - anchor
    row_mean = lax.optimization_barrier(jnp.mean(noisy_field, -1, keepdims=True))
    centred = noisy_field - row_mean
    variance = lax.optimization_barrier(jnp.mean(centred * centred, -1, keepdims=True))
    normed = centred * lax.rsqrt(variance + 1e-06)
    shifts = modulation[:, None, :features]
    scales = modulation[:, None, features:2 * features]
    modulated = (normed * (1.0 + scales) + shifts).astype(jnp.bfloat16)
    return (noisy_field, target, modulated, modulation[:, 2 * features:])

def gelu_tanh(values):
    return jax.nn.gelu(values, approximate=True)

def reference(clean, noise, modulation, strata, up_weight, down_weight):
    fraction, weight = stratum_weights(strata)
    noisy_field, target, modulated, gate_values = modulate(clean, noise, modulation, fraction)
    flat_rows = modulated.reshape(-1, D)
    shard_cols = FFW // N_MP
    output = jnp.zeros((flat_rows.shape[0], D), jnp.float32)
    for shard_index in range(N_MP):
        lower = shard_index * shard_cols
        preact = jnp.dot(flat_rows, up_weight[:, lower:lower + shard_cols], preferred_element_type=jnp.float32)
        hidden = gelu_tanh(preact).astype(jnp.bfloat16)
        partial_value = jnp.dot(hidden, down_weight[lower:lower + shard_cols], preferred_element_type=jnp.float32).astype(jnp.bfloat16)
        partial_value = lax.optimization_barrier(partial_value)
        output = output + partial_value.astype(jnp.float32)
    predicted = noisy_field + gate_values[:, None, :] * output.reshape(SAMPLES, ROWS, D)
    errors = predicted - target
    weight_sum = jnp.sum(weight)
    row_loss = lax.optimization_barrier(jnp.sum(errors * errors, axis=(1, 2))) / (ROWS * D)
    loss_value = jnp.sum(weight * row_loss) / weight_sum
    coefficient = loss_scale * 2.0 * weight / (weight_sum * ROWS * D)
    slopes = (coefficient[:, None, None] * gate_values[:, None, :] * errors).astype(jnp.bfloat16).reshape(-1, D)
    gradients = []
    for shard_index in range(N_MP):
        lower = shard_index * shard_cols
        preact = jnp.dot(flat_rows, up_weight[:, lower:lower + shard_cols], preferred_element_type=jnp.float32)
        hidden_slope = jnp.dot(slopes, down_weight[lower:lower + shard_cols].T, preferred_element_type=jnp.float32)
        unused, pullback = jax.vjp(gelu_tanh, preact)
        pre_slope = pullback(hidden_slope)[0].astype(jnp.bfloat16)
        gradients.append(jnp.dot(pre_slope.T, flat_rows, preferred_element_type=jnp.float32))
    return (jnp.concatenate(gradients, 0), loss_value)
```

```python
import math

import jax
import jax.numpy as jnp
from jax import lax
from jax.sharding import PartitionSpec as P

STRATA = 64


loss_scale = 1048576.0


def stratum_weights(strata):
    quantile = (strata.astype(jnp.float32) + 0.5) / STRATA
    levels = math.sqrt(2.0) * lax.erf_inv(2.0 * quantile - 1.0)
    fraction = jax.nn.sigmoid(levels)
    weight = jnp.exp(-0.5 * levels * levels) / (
        math.sqrt(2.0 * math.pi) * fraction * (1.0 - fraction)
    )
    return (fraction, weight)


def modulate(clean, noise, modulation, fraction):
    features = clean.shape[-1]
    anchor = clean.astype(jnp.float32)
    drift_field = noise.astype(jnp.float32)
    mix_frac = fraction[:, None, None]
    noisy_field = (1.0 - mix_frac) * anchor + mix_frac * drift_field
    target = drift_field - anchor
    row_mean = jnp.mean(noisy_field, -1, keepdims=True)
    centred = noisy_field - row_mean
    variance = jnp.mean(centred * centred, -1, keepdims=True)
    normed = centred * lax.rsqrt(variance + 1e-06)
    shifts = modulation[:, None, :features]
    scales = modulation[:, None, features : 2 * features]
    modulated = (normed * (1.0 + scales) + shifts).astype(jnp.bfloat16)
    return (noisy_field, target, modulated, modulation[:, 2 * features :])


def gelu_tanh(values):
    return jax.nn.gelu(values, approximate=True)


def local_scatter(clean, noise, modulation, strata, up_weight, down_weight):
    samples_here, rows_per, features = clean.shape
    tokens_here = samples_here * rows_per
    fraction, weight = stratum_weights(strata)
    noisy_field, target, modulated, gate_values = modulate(clean, noise, modulation, fraction)
    flat_rows = modulated.reshape(tokens_here, features)
    flat_noisy = noisy_field.reshape(tokens_here, features)
    flat_target = target.reshape(tokens_here, features)
    local_total = jnp.sum(weight)
    grand_total = lax.psum(local_total, "dp")
    preact = jnp.dot(flat_rows, up_weight, preferred_element_type=jnp.float32)
    hidden = gelu_tanh(preact).astype(jnp.bfloat16)
    partial_value = jnp.dot(hidden, down_weight, preferred_element_type=jnp.float32)
    share_rows = tokens_here // lax.axis_size("mp")
    first_row = lax.axis_index("mp") * share_rows
    sample_range = jnp.arange(samples_here, dtype=jnp.int32)
    owners = (first_row + jnp.arange(share_rows, dtype=jnp.int32)) // rows_per
    picker = (owners[:, None] == sample_range[None, :]).astype(jnp.float32)
    own_weight = jnp.dot(picker, weight, precision=lax.Precision.HIGHEST)
    output = lax.psum(partial_value.astype(jnp.bfloat16), "mp").astype(jnp.float32)
    sample_ids = jnp.arange(tokens_here, dtype=jnp.int32) // rows_per
    full_picker = (sample_ids[:, None] == sample_range[None, :]).astype(jnp.float32)
    gate_rows = jnp.dot(full_picker, gate_values, precision=lax.Precision.HIGHEST)
    row_weight = jnp.dot(full_picker, weight, precision=lax.Precision.HIGHEST)
    errors = flat_noisy + gate_rows * output - flat_target
    row_squares = jnp.sum(errors * errors, 1)
    own_squares = lax.dynamic_slice_in_dim(row_squares, first_row, share_rows, 0)
    loss_local = jnp.sum(own_weight * own_squares) / (rows_per * features)
    factor = loss_scale * 2.0 / (grand_total * rows_per * features)
    slopes = (factor * row_weight[:, None] * gate_rows * errors).astype(jnp.bfloat16)
    hidden_slope = lax.dot_general(
        slopes, down_weight, (((1,), (1,)), ((), ())), preferred_element_type=jnp.float32
    )
    unused, pullback = jax.vjp(gelu_tanh, preact)
    pre_slope = pullback(hidden_slope)[0].astype(jnp.bfloat16)
    gradient = lax.psum_scatter(
        lax.dot_general(
            pre_slope, flat_rows, (((0,), (0,)), ((), ())), preferred_element_type=jnp.float32
        ),
        "dp",
        scatter_dimension=0,
        tiled=True,
    )
    loss_sum = lax.psum(loss_local, ("dp", "mp"))
    return (gradient, loss_sum / grand_total)


GATHER_LIMIT_BYTES = 33554432


def local_gather(clean, noise, modulation, strata, up_weight, down_weight):
    samples_here, rows_per, features = clean.shape
    tokens_here = samples_here * rows_per
    fraction, weight = stratum_weights(strata)
    noisy_field, target, modulated, gate_values = modulate(clean, noise, modulation, fraction)
    flat_rows = modulated.reshape(tokens_here, features)
    every_row = lax.all_gather(flat_rows, "dp", axis=0, tiled=True)
    preact = jnp.dot(flat_rows, up_weight, preferred_element_type=jnp.float32)
    hidden = gelu_tanh(preact).astype(jnp.bfloat16)
    partial_value = jnp.dot(hidden, down_weight, preferred_element_type=jnp.float32)
    output = lax.psum(partial_value.astype(jnp.bfloat16), "mp").astype(jnp.float32)
    output = output.reshape(samples_here, rows_per, features)
    gates = gate_values[:, None, :]
    errors = noisy_field + gates * output - target
    squares = jnp.sum(errors * errors, axis=(1, 2)) / (rows_per * features)
    factor = loss_scale * 2.0 / (rows_per * features)
    slopes = (factor * weight[:, None, None] * gates * errors).astype(jnp.bfloat16)
    hidden_slope = lax.dot_general(
        slopes.reshape(tokens_here, features),
        down_weight,
        (((1,), (1,)), ((), ())),
        preferred_element_type=jnp.float32,
    )
    unused, pullback = jax.vjp(gelu_tanh, preact)
    pre_slope = pullback(hidden_slope)[0].astype(jnp.bfloat16)
    own_slope = lax.all_to_all(pre_slope, "dp", split_axis=1, concat_axis=0, tiled=True)
    sums = lax.psum(jnp.stack([jnp.sum(weight * squares), jnp.sum(weight)]), "dp")
    gradient = lax.dot_general(
        own_slope, every_row, (((0,), (0,)), ((), ())), preferred_element_type=jnp.float32
    )
    return (gradient / sums[1], sums[0] / sums[1])


def local(clean, *others):
    gathered = lax.axis_size("dp") * clean.size * clean.dtype.itemsize
    body = local_gather if gathered <= GATHER_LIMIT_BYTES else local_scatter
    return body(clean, *others)


def solution(mesh):
    return jax.shard_map(
        local,
        mesh=mesh,
        in_specs=(
            P("dp", None, None),
            P("dp", None, None),
            P("dp", None),
            P("dp"),
            P(None, "mp"),
            P("mp", None),
        ),
        out_specs=(P(("mp", "dp"), None), P()),
        check_vma=False,
    )
```

```python
import functools
import math

import jax
import jax.numpy as jnp
from jax import lax
from jax.experimental import pallas as pl
from jax.experimental.pallas import tpu as pltpu
from jax.sharding import PartitionSpec as P

STRATA = 64


loss_scale = 1048576.0


def stratum_weights(strata):
    quantile = (strata.astype(jnp.float32) + 0.5) / STRATA
    levels = math.sqrt(2.0) * lax.erf_inv(2.0 * quantile - 1.0)
    fraction = jax.nn.sigmoid(levels)
    weight = jnp.exp(-0.5 * levels * levels) / (
        math.sqrt(2.0 * math.pi) * fraction * (1.0 - fraction)
    )
    return (fraction, weight)


def modulate(clean, noise, modulation, fraction):
    features = clean.shape[-1]
    anchor = clean.astype(jnp.float32)
    drift_field = noise.astype(jnp.float32)
    mix_frac = fraction[:, None, None]
    noisy_field = (1.0 - mix_frac) * anchor + mix_frac * drift_field
    target = drift_field - anchor
    row_mean = jnp.mean(noisy_field, -1, keepdims=True)
    centred = noisy_field - row_mean
    variance = jnp.mean(centred * centred, -1, keepdims=True)
    normed = centred * lax.rsqrt(variance + 1e-06)
    shifts = modulation[:, None, :features]
    scales = modulation[:, None, features : 2 * features]
    modulated = (normed * (1.0 + scales) + shifts).astype(jnp.bfloat16)
    return (noisy_field, target, modulated, modulation[:, 2 * features :])


def gelu_tanh(values):
    return jax.nn.gelu(values, approximate=True)


def local_scatter(clean, noise, modulation, strata, up_weight, down_weight):
    samples_here, rows_per, features = clean.shape
    tokens_here = samples_here * rows_per
    fraction, weight = stratum_weights(strata)
    noisy_field, target, modulated, gate_values = modulate(clean, noise, modulation, fraction)
    flat_rows = modulated.reshape(tokens_here, features)
    flat_noisy = noisy_field.reshape(tokens_here, features)
    flat_target = target.reshape(tokens_here, features)
    local_total = jnp.sum(weight)
    grand_total = lax.psum(local_total, "dp")
    preact = jnp.dot(flat_rows, up_weight, preferred_element_type=jnp.float32)
    hidden = gelu_tanh(preact).astype(jnp.bfloat16)
    partial_value = jnp.dot(hidden, down_weight, preferred_element_type=jnp.float32)
    share_rows = tokens_here // lax.axis_size("mp")
    first_row = lax.axis_index("mp") * share_rows
    sample_range = jnp.arange(samples_here, dtype=jnp.int32)
    owners = (first_row + jnp.arange(share_rows, dtype=jnp.int32)) // rows_per
    picker = (owners[:, None] == sample_range[None, :]).astype(jnp.float32)
    own_weight = jnp.dot(picker, weight, precision=lax.Precision.HIGHEST)
    output = lax.psum(partial_value.astype(jnp.bfloat16), "mp").astype(jnp.float32)
    sample_ids = jnp.arange(tokens_here, dtype=jnp.int32) // rows_per
    full_picker = (sample_ids[:, None] == sample_range[None, :]).astype(jnp.float32)
    gate_rows = jnp.dot(full_picker, gate_values, precision=lax.Precision.HIGHEST)
    row_weight = jnp.dot(full_picker, weight, precision=lax.Precision.HIGHEST)
    errors = flat_noisy + gate_rows * output - flat_target
    row_squares = jnp.sum(errors * errors, 1)
    own_squares = lax.dynamic_slice_in_dim(row_squares, first_row, share_rows, 0)
    loss_local = jnp.sum(own_weight * own_squares) / (rows_per * features)
    factor = loss_scale * 2.0 / (grand_total * rows_per * features)
    slopes = (factor * row_weight[:, None] * gate_rows * errors).astype(jnp.bfloat16)
    hidden_slope = lax.dot_general(
        slopes, down_weight, (((1,), (1,)), ((), ())), preferred_element_type=jnp.float32
    )
    unused, pullback = jax.vjp(gelu_tanh, preact)
    pre_slope = pullback(hidden_slope)[0].astype(jnp.bfloat16)
    gradient = lax.psum_scatter(
        lax.dot_general(
            pre_slope, flat_rows, (((0,), (0,)), ((), ())), preferred_element_type=jnp.float32
        ),
        "dp",
        scatter_dimension=0,
        tiled=True,
    )
    loss_sum = lax.psum(loss_local, ("dp", "mp"))
    return (gradient, loss_sum / grand_total)


GATHER_LIMIT_BYTES = 33554432


def local_gather(clean, noise, modulation, strata, up_weight, down_weight):
    samples_here, rows_per, features = clean.shape
    tokens_here = samples_here * rows_per
    fraction, weight = stratum_weights(strata)
    noisy_field, target, modulated, gate_values = modulate(clean, noise, modulation, fraction)
    flat_rows = modulated.reshape(tokens_here, features)
    every_row = lax.all_gather(flat_rows, "dp", axis=0, tiled=True)
    preact = jnp.dot(flat_rows, up_weight, preferred_element_type=jnp.float32)
    hidden = gelu_tanh(preact).astype(jnp.bfloat16)
    partial_value = jnp.dot(hidden, down_weight, preferred_element_type=jnp.float32)
    output = lax.psum(partial_value.astype(jnp.bfloat16), "mp").astype(jnp.float32)
    output = output.reshape(samples_here, rows_per, features)
    gates = gate_values[:, None, :]
    errors = noisy_field + gates * output - target
    squares = jnp.sum(errors * errors, axis=(1, 2)) / (rows_per * features)
    factor = loss_scale * 2.0 / (rows_per * features)
    slopes = (factor * weight[:, None, None] * gates * errors).astype(jnp.bfloat16)
    hidden_slope = lax.dot_general(
        slopes.reshape(tokens_here, features),
        down_weight,
        (((1,), (1,)), ((), ())),
        preferred_element_type=jnp.float32,
    )
    unused, pullback = jax.vjp(gelu_tanh, preact)
    pre_slope = pullback(hidden_slope)[0].astype(jnp.bfloat16)
    own_slope = lax.all_to_all(pre_slope, "dp", split_axis=1, concat_axis=0, tiled=True)
    sums = lax.psum(jnp.stack([jnp.sum(weight * squares), jnp.sum(weight)]), "dp")
    gradient = lax.dot_general(
        own_slope, every_row, (((0,), (0,)), ((), ())), preferred_element_type=jnp.float32
    )
    return (gradient / sums[1], sums[0] / sums[1])


MESH = pl.DeviceIdType.MESH
CHUNK = 16
LANES = 128
CORES = 2


def gelu_slope(x):
    k = math.sqrt(2.0 / math.pi)
    t = jnp.tanh(k * (x + 0.044715 * (x * x * x)))
    return 0.5 * (1.0 + t) + 0.5 * x * (1.0 - t * t) * (k * (1.0 + 3.0 * 0.044715 * x * x))


def step_kernel(
    sizes,
    frac_ref,
    weight_ref,
    clean_ref,
    noise_ref,
    modulation_ref,
    up_hbm,
    down_hbm,
    grad_ref,
    sums_ref,
    up,
    down,
    rows_all,
    preact,
    slope_t,
    hidden,
    part_out,
    part_in,
    part_own,
    chip_sum,
    slopes,
    pre_out,
    pre_in,
    core_tile,
    all_tile,
    load_sem,
    rows_send,
    rows_recv,
    part_sem,
    chip_send,
    chip_recv,
    slopes_sem,
    core_sem,
    pre_send,
    pre_recv,
    tile_send,
    tile_recv,
):
    nz, ny, nx, rows_per = sizes
    ndp = nz * ny
    samples, features = clean_ref.shape[0] // rows_per, clean_ref.shape[1]
    units = up.shape[1]
    half = clean_ref.shape[0] // CORES
    share = units // ndp
    kinds = 3 + (ny - 1)
    me, group = lax.axis_index("dp"), lax.axis_index("mp")
    z, y = me // ny, lax.rem(me, ny)
    x, core = group // CORES, lax.rem(group, CORES)
    mate = (me, x * CORES + 1 - core)
    own_rows = pl.ds(pl.multiple_of(core * half, half), half)
    mate_rows = pl.ds(pl.multiple_of((1 - core) * half, half), half)

    load_up = pltpu.make_async_copy(up_hbm, up, load_sem.at[0])
    load_down = pltpu.make_async_copy(down_hbm, down, load_sem.at[1])
    load_up.start()
    load_down.start()

    others = [(lax.rem(me + k, ndp), group) for k in range(1, ndp)]
    across = [lax.rem(x + k, nx) for k in range(1, nx)]
    barrier = pltpu.get_barrier_semaphore()
    partners = others + [(me, p * CORES + core) for p in across] + [mate]
    for partner in partners:
        pl.semaphore_signal(barrier, inc=1, device_id=partner, device_id_type=MESH)

    def remote(src, dst, send_sem, recv_sem, device):
        return pltpu.make_async_remote_copy(
            src_ref=src,
            dst_ref=dst,
            send_sem=send_sem,
            recv_sem=recv_sem,
            device_id=device,
            device_id_type=MESH,
        )

    def piece(block, side, kind, device):
        rows = rows_all.at[block, pl.ds(pl.multiple_of(side * half, half), half)]
        return remote(
            rows,
            rows,
            rows_send.at[block * kinds + kind],
            rows_recv.at[block * CORES + side],
            device,
        )

    def to_z(block, kind):
        return piece(block, core, kind, (me - ny if kind == 0 else me + ny, group))

    def to_y(block):
        return [
            piece(block, core, 3 + k - 1, (z * ny + lax.rem(y + k, ny), group))
            for k in range(1, ny)
        ]

    def to_mate(block):
        return piece(block, core, 2, mate)

    def walk_z(k, act):
        @pl.when(z + k < nz)
        def from_above():
            block = me + k * ny
            act(block, 0, z > 0)

        @pl.when(z - k >= 0)
        def from_below():
            block = me - k * ny
            act(block, 1, z < nz - 1)

    def relay(block, kind, onward):
        to_mate(block).wait_recv()

        @pl.when(onward)
        def pass_on():
            to_z(block, kind).start()

        for copy in to_y(block):
            copy.start()
        to_mate(block).start()

    def drain(block, kind, onward):
        @pl.when(onward)
        def sent():
            to_z(block, kind).wait_send()

        for copy in to_y(block):
            copy.wait_send()
        to_mate(block).wait_send()

    def walk_y(k, act):
        for j in range(1, ny):
            column = lax.rem(y + j, ny)
            if k == 0:
                act(z * ny + column)
            else:

                @pl.when(z + k < nz)
                def above():
                    act((z + k) * ny + column)

                @pl.when(z - k >= 0)
                def below():
                    act((z - k) * ny + column)

    def share_y(block):
        to_mate(block).wait_recv()
        to_mate(block).start()

    def mix(rows, sample):
        fraction = frac_ref[sample]
        anchor = clean_ref[rows].astype(jnp.float32)
        drift = noise_ref[rows].astype(jnp.float32)
        return (1.0 - fraction) * anchor + fraction * drift, drift - anchor

    def modulate_rows(base):
        def step(i, carry):
            first = pl.multiple_of(base + i * CHUNK, CHUNK)
            rows = pl.ds(first, CHUNK)
            sample = first // rows_per
            noisy, unused = mix(rows, sample)
            centred = noisy - jnp.mean(noisy, -1, keepdims=True)
            variance = jnp.mean(centred * centred, -1, keepdims=True)
            normed = centred * lax.rsqrt(variance + 1e-06)
            shift = modulation_ref[pl.ds(sample, 1), :features]
            scale = modulation_ref[pl.ds(sample, 1), features : 2 * features]
            rows_all[me, rows] = (normed * (1.0 + scale) + shift).astype(jnp.bfloat16)
            return carry

        lax.fori_loop(0, half // CHUNK, step, 0)

    modulate_rows(core * half)
    modulate_rows((1 - core) * half)
    pl.semaphore_wait(barrier, len(partners))

    @pl.when(z > 0)
    def first_down():
        to_z(me, 0).start()

    @pl.when(z < nz - 1)
    def first_up():
        to_z(me, 1).start()

    for copy in to_y(me):
        copy.start()

    preact[:, (units // LANES) * LANES :] = jnp.zeros(
        (preact.shape[0], preact.shape[1] - (units // LANES) * LANES), jnp.float32
    )
    load_up.wait()
    preact[:, :units] = jnp.dot(rows_all[me], up[...], preferred_element_type=jnp.float32)
    values = preact[:, :units]
    hidden[...] = jax.nn.gelu(values, approximate=True).astype(jnp.bfloat16)
    load_down.wait()
    part_out[...] = jnp.dot(
        hidden[mate_rows], down[...], preferred_element_type=jnp.float32
    ).astype(jnp.bfloat16)
    part_copy = remote(part_out, part_in, part_sem.at[0], part_sem.at[1], mate)
    part_copy.start()
    part_own[...] = jnp.dot(hidden[own_rows], down[...], preferred_element_type=jnp.float32)
    part_copy.wait_recv()
    chip_sum[x] = (part_own[...] + part_in[...].astype(jnp.float32)).astype(jnp.bfloat16)
    chip_copies = [
        remote(
            chip_sum.at[x],
            chip_sum.at[x],
            chip_send.at[p],
            chip_recv.at[x],
            (me, p * CORES + core),
        )
        for p in across
    ]
    for copy in chip_copies:
        copy.start()

    for j in range(preact.shape[1] // LANES):
        block = preact[:, j * LANES : (j + 1) * LANES]
        slope_t[j * LANES : (j + 1) * LANES, :] = gelu_slope(block).T

    if nz > 1:
        walk_z(1, relay)

    for p in across:
        remote(
            chip_sum.at[p], chip_sum.at[p], chip_send.at[p], chip_recv.at[p], mate
        ).wait_recv()

    scale_all = loss_scale * 2.0 / (rows_per * features)

    def slope_step(i, total):
        first = pl.multiple_of(core * half + i * CHUNK, CHUNK)
        rows = pl.ds(first, CHUNK)
        here = pl.ds(pl.multiple_of(i * CHUNK, CHUNK), CHUNK)
        sample = first // rows_per
        noisy, target = mix(rows, sample)
        output = chip_sum[0, here].astype(jnp.float32)
        for p in range(1, nx):
            output = output + chip_sum[p, here].astype(jnp.float32)
        gate = modulation_ref[pl.ds(sample, 1), 2 * features :]
        errors = noisy + gate * output - target
        weight = weight_ref[sample]
        slopes[rows] = (scale_all * weight * gate * errors).astype(jnp.bfloat16)
        return total + weight * jnp.sum(errors * errors, -1, keepdims=True)

    squares = lax.fori_loop(0, half // CHUNK, slope_step, jnp.zeros((CHUNK, 1), jnp.float32))
    own_slopes = slopes.at[own_rows]
    slopes_copy = remote(own_slopes, own_slopes, slopes_sem.at[0], slopes_sem.at[1], mate)
    slopes_copy.start()
    loss_part = jnp.sum(squares) / (rows_per * features)
    core_tile[core] = jnp.full((8, LANES), loss_part, jnp.float32)
    core_copy = remote(
        core_tile.at[core], core_tile.at[core], core_sem.at[0], core_sem.at[1], mate
    )
    core_copy.start()
    slopes_copy.wait_recv()

    slope_all = lax.dot_general(
        down[...], slopes[...], (((1,), (1,)), ((), ())), preferred_element_type=jnp.float32
    )
    for d in range(ndp):
        part = slice(d * share, (d + 1) * share)
        pre_out[d] = (slope_all[part] * slope_t[part, :]).astype(jnp.bfloat16)
    pre_in[me] = pre_out[me]
    pre_copies = [
        remote(pre_out.at[peer[0]], pre_in.at[me], pre_send.at[peer[0]], pre_recv.at[me], peer)
        for peer in others
    ]
    for copy in pre_copies:
        copy.start()

    core_copy.wait_recv()
    weight_here = weight_ref[0]
    for sample in range(1, samples):
        weight_here = weight_here + weight_ref[sample]
    line = lax.broadcasted_iota(jnp.int32, (8, LANES), 0)
    all_tile[me] = jnp.where(line == 0, core_tile[0] + core_tile[1], weight_here)
    tile_copies = [
        remote(all_tile.at[me], all_tile.at[me], tile_send.at[peer[0]], tile_recv.at[me], peer)
        for peer in others
    ]
    for copy in tile_copies:
        copy.start()

    walk_y(0, share_y)
    for k in range(2, nz):
        walk_y(k - 1, share_y)
        walk_z(k, relay)
    if nz > 1:
        walk_y(nz - 1, share_y)

    grad_ref[...] = jnp.dot(pre_in[me], rows_all[me], preferred_element_type=jnp.float32)

    def grad_step(k, carry):
        block = lax.rem(me + k, ndp)
        piece(block, 1 - core, 2, mate).wait_recv()
        remote(
            pre_out.at[block], pre_in.at[block], pre_send.at[block], pre_recv.at[block], mate
        ).wait_recv()
        grad_ref[...] += jnp.dot(
            pre_in[block], rows_all[block], preferred_element_type=jnp.float32
        )
        return carry

    lax.fori_loop(1, ndp, grad_step, 0)

    for peer in others:
        block = peer[0]
        remote(
            all_tile.at[block], all_tile.at[block], tile_send.at[block], tile_recv.at[block], peer
        ).wait_recv()
    sums = all_tile[0]
    for d in range(1, ndp):
        sums = sums + all_tile[d]
    sums_ref[...] = sums

    @pl.when(z > 0)
    def first_down_sent():
        to_z(me, 0).wait_send()

    @pl.when(z < nz - 1)
    def first_up_sent():
        to_z(me, 1).wait_send()

    for copy in to_y(me) + [part_copy, slopes_copy, core_copy]:
        copy.wait_send()
    for copy in chip_copies + pre_copies + tile_copies:
        copy.wait_send()
    for k in range(1, nz):
        walk_z(k, drain)
    for k in range(nz):
        walk_y(k, lambda block: to_mate(block).wait_send())


def local_kernel(sizes, clean, noise, modulation, strata, up_weight, down_weight):
    samples_here, rows_per, features = clean.shape
    nz, ny, nx = sizes
    ndp, tokens, units = nz * ny, samples_here * rows_per, up_weight.shape[1]
    half, share, padded = tokens // CORES, units // ndp, pl.cdiv(units, LANES) * LANES
    fraction, weight = stratum_weights(strata)
    bf16, f32 = jnp.bfloat16, jnp.float32
    vmem = pl.BlockSpec(memory_space=pltpu.VMEM)
    smem = pl.BlockSpec(memory_space=pltpu.SMEM)
    anywhere = pl.BlockSpec(memory_space=pl.ANY)
    dma = pltpu.SemaphoreType.DMA
    gradient, sums = pl.pallas_call(
        functools.partial(step_kernel, (nz, ny, nx, rows_per)),
        out_shape=(
            jax.ShapeDtypeStruct((share, features), f32),
            jax.ShapeDtypeStruct((8, LANES), f32),
        ),
        in_specs=[smem, smem, vmem, vmem, vmem, anywhere, anywhere],
        out_specs=(vmem, vmem),
        scratch_shapes=[
            pltpu.VMEM((features, units), bf16),
            pltpu.VMEM((units, features), bf16),
            pltpu.VMEM((ndp, tokens, features), bf16),
            pltpu.VMEM((tokens, padded), f32),
            pltpu.VMEM((padded, tokens), f32),
            pltpu.VMEM((tokens, units), bf16),
            pltpu.VMEM((half, features), bf16),
            pltpu.VMEM((half, features), bf16),
            pltpu.VMEM((half, features), f32),
            pltpu.VMEM((nx, half, features), bf16),
            pltpu.VMEM((tokens, features), bf16),
            pltpu.VMEM((ndp, share, tokens), bf16),
            pltpu.VMEM((ndp, share, tokens), bf16),
            pltpu.VMEM((CORES, 8, LANES), f32),
            pltpu.VMEM((ndp, 8, LANES), f32),
            dma((2,)),
            dma((ndp * (2 + ny),)),
            dma((ndp * CORES,)),
            dma((2,)),
            dma((nx,)),
            dma((nx,)),
            dma((2,)),
            dma((2,)),
            dma((ndp,)),
            dma((ndp,)),
            dma((ndp,)),
            dma((ndp,)),
        ],
        compiler_params=pltpu.CompilerParams(
            collective_id=0, has_side_effects=True, vmem_limit_bytes=60 * 1024 * 1024
        ),
    )(
        fraction,
        weight,
        clean.reshape(tokens, features),
        noise.reshape(tokens, features),
        modulation,
        up_weight,
        down_weight,
    )
    return (gradient / sums[1, 0], sums[0, 0] / sums[1, 0])


def chip_sizes(mesh):
    if mesh.shape["mp"] % CORES:
        return None
    spots = [tuple(d.coords) for d in mesh.devices[:, 0]]
    ny = len({spot[1] for spot in spots})
    return (mesh.shape["dp"] // ny, ny, mesh.shape["mp"] // CORES)


def local(sizes, clean, *others):
    gathered = lax.axis_size("dp") * clean.size * clean.dtype.itemsize
    units = others[-1].shape[0]
    half = clean.shape[0] * clean.shape[1] // CORES
    if gathered > GATHER_LIMIT_BYTES:
        return local_scatter(clean, *others)
    if units % (8 * lax.axis_size("dp")) or half % LANES or clean.shape[1] % CHUNK:
        return local_gather(clean, *others)
    return local_kernel(sizes, clean, *others)


def solution(mesh):
    return jax.shard_map(
        functools.partial(local, chip_sizes(mesh)),
        mesh=mesh,
        in_specs=(
            P("dp", None, None),
            P("dp", None, None),
            P("dp", None),
            P("dp"),
            P(None, "mp"),
            P("mp", None),
        ),
        out_specs=(P(("mp", "dp"), None), P()),
        check_vma=False,
    )
```

```python
import functools
import math

import jax
import jax.numpy as jnp
from jax import lax
from jax.experimental import pallas as pl
from jax.experimental.pallas import tpu as pltpu
from jax.sharding import PartitionSpec as P

STRATA = 64


loss_scale = 1048576.0


def stratum_weights(strata):
    quantile = (strata.astype(jnp.float32) + 0.5) / STRATA
    levels = math.sqrt(2.0) * lax.erf_inv(2.0 * quantile - 1.0)
    fraction = jax.nn.sigmoid(levels)
    weight = jnp.exp(-0.5 * levels * levels) / (
        math.sqrt(2.0 * math.pi) * fraction * (1.0 - fraction)
    )
    return (fraction, weight)


def modulate(clean, noise, modulation, fraction):
    features = clean.shape[-1]
    anchor = clean.astype(jnp.float32)
    drift_field = noise.astype(jnp.float32)
    mix_frac = fraction[:, None, None]
    noisy_field = (1.0 - mix_frac) * anchor + mix_frac * drift_field
    target = drift_field - anchor
    row_mean = jnp.mean(noisy_field, -1, keepdims=True)
    centred = noisy_field - row_mean
    variance = jnp.mean(centred * centred, -1, keepdims=True)
    normed = centred * lax.rsqrt(variance + 1e-06)
    shifts = modulation[:, None, :features]
    scales = modulation[:, None, features : 2 * features]
    modulated = (normed * (1.0 + scales) + shifts).astype(jnp.bfloat16)
    return (noisy_field, target, modulated, modulation[:, 2 * features :])


def gelu_tanh(values):
    return jax.nn.gelu(values, approximate=True)


def local_scatter(clean, noise, modulation, strata, up_weight, down_weight):
    samples_here, rows_per, features = clean.shape
    tokens_here = samples_here * rows_per
    fraction, weight = stratum_weights(strata)
    noisy_field, target, modulated, gate_values = modulate(clean, noise, modulation, fraction)
    flat_rows = modulated.reshape(tokens_here, features)
    flat_noisy = noisy_field.reshape(tokens_here, features)
    flat_target = target.reshape(tokens_here, features)
    local_total = jnp.sum(weight)
    grand_total = lax.psum(local_total, "dp")
    preact = jnp.dot(flat_rows, up_weight, preferred_element_type=jnp.float32)
    hidden = gelu_tanh(preact).astype(jnp.bfloat16)
    partial_value = jnp.dot(hidden, down_weight, preferred_element_type=jnp.float32)
    share_rows = tokens_here // lax.axis_size("mp")
    first_row = lax.axis_index("mp") * share_rows
    sample_range = jnp.arange(samples_here, dtype=jnp.int32)
    owners = (first_row + jnp.arange(share_rows, dtype=jnp.int32)) // rows_per
    picker = (owners[:, None] == sample_range[None, :]).astype(jnp.float32)
    own_weight = jnp.dot(picker, weight, precision=lax.Precision.HIGHEST)
    output = lax.psum(partial_value.astype(jnp.bfloat16), "mp").astype(jnp.float32)
    sample_ids = jnp.arange(tokens_here, dtype=jnp.int32) // rows_per
    full_picker = (sample_ids[:, None] == sample_range[None, :]).astype(jnp.float32)
    gate_rows = jnp.dot(full_picker, gate_values, precision=lax.Precision.HIGHEST)
    row_weight = jnp.dot(full_picker, weight, precision=lax.Precision.HIGHEST)
    errors = flat_noisy + gate_rows * output - flat_target
    row_squares = jnp.sum(errors * errors, 1)
    own_squares = lax.dynamic_slice_in_dim(row_squares, first_row, share_rows, 0)
    loss_local = jnp.sum(own_weight * own_squares) / (rows_per * features)
    factor = loss_scale * 2.0 / (grand_total * rows_per * features)
    slopes = (factor * row_weight[:, None] * gate_rows * errors).astype(jnp.bfloat16)
    hidden_slope = lax.dot_general(
        slopes, down_weight, (((1,), (1,)), ((), ())), preferred_element_type=jnp.float32
    )
    unused, pullback = jax.vjp(gelu_tanh, preact)
    pre_slope = pullback(hidden_slope)[0].astype(jnp.bfloat16)
    gradient = lax.psum_scatter(
        lax.dot_general(
            pre_slope, flat_rows, (((0,), (0,)), ((), ())), preferred_element_type=jnp.float32
        ),
        "dp",
        scatter_dimension=0,
        tiled=True,
    )
    loss_sum = lax.psum(loss_local, ("dp", "mp"))
    return (gradient, loss_sum / grand_total)


GATHER_LIMIT_BYTES = 33554432


def local_gather(clean, noise, modulation, strata, up_weight, down_weight):
    samples_here, rows_per, features = clean.shape
    tokens_here = samples_here * rows_per
    fraction, weight = stratum_weights(strata)
    noisy_field, target, modulated, gate_values = modulate(clean, noise, modulation, fraction)
    flat_rows = modulated.reshape(tokens_here, features)
    every_row = lax.all_gather(flat_rows, "dp", axis=0, tiled=True)
    preact = jnp.dot(flat_rows, up_weight, preferred_element_type=jnp.float32)
    hidden = gelu_tanh(preact).astype(jnp.bfloat16)
    partial_value = jnp.dot(hidden, down_weight, preferred_element_type=jnp.float32)
    output = lax.psum(partial_value.astype(jnp.bfloat16), "mp").astype(jnp.float32)
    output = output.reshape(samples_here, rows_per, features)
    gates = gate_values[:, None, :]
    errors = noisy_field + gates * output - target
    squares = jnp.sum(errors * errors, axis=(1, 2)) / (rows_per * features)
    factor = loss_scale * 2.0 / (rows_per * features)
    slopes = (factor * weight[:, None, None] * gates * errors).astype(jnp.bfloat16)
    hidden_slope = lax.dot_general(
        slopes.reshape(tokens_here, features),
        down_weight,
        (((1,), (1,)), ((), ())),
        preferred_element_type=jnp.float32,
    )
    unused, pullback = jax.vjp(gelu_tanh, preact)
    pre_slope = pullback(hidden_slope)[0].astype(jnp.bfloat16)
    own_slope = lax.all_to_all(pre_slope, "dp", split_axis=1, concat_axis=0, tiled=True)
    sums = lax.psum(jnp.stack([jnp.sum(weight * squares), jnp.sum(weight)]), "dp")
    gradient = lax.dot_general(
        own_slope, every_row, (((0,), (0,)), ((), ())), preferred_element_type=jnp.float32
    )
    return (gradient / sums[1], sums[0] / sums[1])


MESH = pl.DeviceIdType.MESH
CHUNK = 16
LANES = 128
CORES = 2


def gelu_slope(x):
    k = math.sqrt(2.0 / math.pi)
    t = jnp.tanh(k * (x + 0.044715 * (x * x * x)))
    return 0.5 * (1.0 + t) + 0.5 * x * (1.0 - t * t) * (k * (1.0 + 3.0 * 0.044715 * x * x))


def step_kernel(
    sizes,
    frac_ref,
    weight_ref,
    clean_ref,
    noise_ref,
    modulation_ref,
    up_hbm,
    down_hbm,
    grad_ref,
    sums_ref,
    up,
    down,
    rows_all,
    preact,
    slope_t,
    hidden,
    part_out,
    part_in,
    part_own,
    chip_sum,
    slopes,
    pre_out,
    pre_in,
    core_tile,
    all_tile,
    load_sem,
    rows_send,
    rows_recv,
    part_sem,
    chip_send,
    chip_recv,
    slopes_sem,
    core_sem,
    pre_send,
    pre_recv,
    tile_send,
    tile_recv,
):
    nz, ny, nx, rows_per = sizes
    ndp = nz * ny
    samples, features = clean_ref.shape[0] // rows_per, clean_ref.shape[1]
    units = up.shape[0]
    half = clean_ref.shape[0] // CORES
    share = units // ndp
    strip = half // nx
    kinds = 2 + CORES * nx + (ny - 1) + (nx - 1)
    me, group = lax.axis_index("dp"), lax.axis_index("mp")
    z, y = me // ny, lax.rem(me, ny)
    x, core = group // CORES, lax.rem(group, CORES)
    mate = (me, x * CORES + 1 - core)
    own_rows = pl.ds(pl.multiple_of(core * half, half), half)
    mate_rows = pl.ds(pl.multiple_of((1 - core) * half, half), half)

    load_up = pltpu.make_async_copy(up_hbm, up, load_sem.at[0])
    load_down = pltpu.make_async_copy(down_hbm, down, load_sem.at[1])
    load_up.start()
    load_down.start()

    others = [(lax.rem(me + k, ndp), group) for k in range(1, ndp)]
    across = [lax.rem(x + k, nx) for k in range(1, nx)]
    barrier = pltpu.get_barrier_semaphore()
    partners = others + [(me, p * CORES + core) for p in across] + [mate]
    for partner in partners:
        pl.semaphore_signal(barrier, inc=1, device_id=partner, device_id_type=MESH)

    def remote(src, dst, send_sem, recv_sem, device):
        return pltpu.make_async_remote_copy(
            src_ref=src,
            dst_ref=dst,
            send_sem=send_sem,
            recv_sem=recv_sem,
            device_id=device,
            device_id_type=MESH,
        )

    mate_kind, y_kind = 2, 2 + nx
    x_kind = y_kind + ny - 1

    def copy_rows(block, first, count, kind, arrival, device):
        rows = rows_all.at[block, pl.ds(pl.multiple_of(first, count), count)]
        return remote(
            rows,
            rows,
            rows_send.at[block * kinds + kind],
            rows_recv.at[block * CORES * nx + arrival],
            device,
        )

    def piece(block, side, kind, device):
        return copy_rows(block, side * half, half, kind, side * nx, device)

    def strip_of(block, side, lane, kind, device):
        first = side * half + lane * strip
        return copy_rows(block, first, strip, kind, side * nx + lane, device)

    def to_z(block, kind):
        return piece(block, core, kind, (me - ny if kind == 0 else me + ny, group))

    def to_y(block):
        return [
            strip_of(block, core, x, y_kind + k - 1, (z * ny + lax.rem(y + k, ny), group))
            for k in range(1, ny)
        ]

    def to_x(block):
        return [
            strip_of(block, core, x, x_kind + k - 1, (me, lax.rem(x + k, nx) * CORES + core))
            for k in range(1, nx)
        ]

    def to_mate(block):
        return piece(block, core, mate_kind, mate)

    def strip_to_mate(block, lane):
        return strip_of(block, core, lane, mate_kind + lane, mate)

    def walk_z(k, act):
        @pl.when(z + k < nz)
        def from_above():
            act(me + k * ny, 0, z > 0)

        @pl.when(z - k >= 0)
        def from_below():
            act(me - k * ny, 1, z < nz - 1)

    def relay(block, kind, onward):
        to_mate(block).wait_recv()

        @pl.when(onward)
        def pass_on():
            to_z(block, kind).start()

        for copy in to_y(block):
            copy.start()
        to_mate(block).start()

    def drain(block, kind, onward):
        @pl.when(onward)
        def sent():
            to_z(block, kind).wait_send()

        for copy in to_y(block):
            copy.wait_send()
        to_mate(block).wait_send()

    def walk_y(k, act):
        for j in range(1, ny):
            column = lax.rem(y + j, ny)
            if k == 0:
                act(z * ny + column)
            else:

                @pl.when(z + k < nz)
                def above():
                    act((z + k) * ny + column)

                @pl.when(z - k >= 0)
                def below():
                    act((z - k) * ny + column)

    def share_y(block):
        strip_to_mate(block, x).wait_recv()
        for copy in to_x(block):
            copy.start()
        strip_to_mate(block, x).start()

    def share_x(block):
        for p in across:
            strip_to_mate(block, p).wait_recv()
            strip_to_mate(block, p).start()

    def drain_y(block):
        for copy in to_x(block):
            copy.wait_send()
        for lane in range(nx):
            strip_to_mate(block, lane).wait_send()

    def await_own_column(block):
        piece(block, 1 - core, mate_kind, mate).wait_recv()

    def await_other_column(block):
        for lane in range(nx):
            strip_of(block, 1 - core, lane, mate_kind, mate).wait_recv()

    def mix(rows, sample):
        fraction = frac_ref[sample]
        anchor = clean_ref[rows].astype(jnp.float32)
        drift = noise_ref[rows].astype(jnp.float32)
        return (1.0 - fraction) * anchor + fraction * drift, drift - anchor

    def modulate_rows(base):
        def step(i, carry):
            first = pl.multiple_of(base + i * CHUNK, CHUNK)
            rows = pl.ds(first, CHUNK)
            sample = first // rows_per
            noisy, unused = mix(rows, sample)
            centred = noisy - jnp.mean(noisy, -1, keepdims=True)
            variance = jnp.mean(centred * centred, -1, keepdims=True)
            normed = centred * lax.rsqrt(variance + 1e-06)
            shift = modulation_ref[pl.ds(sample, 1), :features]
            scale = modulation_ref[pl.ds(sample, 1), features : 2 * features]
            rows_all[me, rows] = (normed * (1.0 + scale) + shift).astype(jnp.bfloat16)
            return carry

        lax.fori_loop(0, half // CHUNK, step, 0)

    modulate_rows(core * half)
    modulate_rows((1 - core) * half)
    pl.semaphore_wait(barrier, len(partners))

    @pl.when(z > 0)
    def first_down():
        to_z(me, 0).start()

    @pl.when(z < nz - 1)
    def first_up():
        to_z(me, 1).start()

    for copy in to_y(me):
        copy.start()

    tail = (units // LANES) * LANES
    preact[tail:, :] = jnp.zeros((preact.shape[0] - tail, preact.shape[1]), jnp.float32)
    load_up.wait()
    preact[:units, :] = lax.dot_general(
        up[...], rows_all[me], (((1,), (1,)), ((), ())), preferred_element_type=jnp.float32
    )
    for j in range(preact.shape[0] // LANES):
        part = slice(j * LANES, (j + 1) * LANES)
        values = jax.nn.gelu(preact[part, :], approximate=True)
        hidden[:, part] = values.T.astype(jnp.bfloat16)
    load_down.wait()
    part_out[...] = jnp.dot(
        hidden[mate_rows, :units], down[...], preferred_element_type=jnp.float32
    ).astype(jnp.bfloat16)
    part_copy = remote(part_out, part_in, part_sem.at[0], part_sem.at[1], mate)
    part_copy.start()
    part_own[...] = jnp.dot(hidden[own_rows, :units], down[...], preferred_element_type=jnp.float32)
    part_copy.wait_recv()
    chip_sum[x] = (part_own[...] + part_in[...].astype(jnp.float32)).astype(jnp.bfloat16)
    chip_copies = [
        remote(
            chip_sum.at[x],
            chip_sum.at[x],
            chip_send.at[p],
            chip_recv.at[x],
            (me, p * CORES + core),
        )
        for p in across
    ]
    for copy in chip_copies:
        copy.start()

    slope_t[...] = gelu_slope(preact[...])

    if nz > 1:
        walk_z(1, relay)

    for p in across:
        remote(
            chip_sum.at[p], chip_sum.at[p], chip_send.at[p], chip_recv.at[p], mate
        ).wait_recv()

    scale_all = loss_scale * 2.0 / (rows_per * features)

    def slope_step(i, total):
        first = pl.multiple_of(core * half + i * CHUNK, CHUNK)
        rows = pl.ds(first, CHUNK)
        here = pl.ds(pl.multiple_of(i * CHUNK, CHUNK), CHUNK)
        sample = first // rows_per
        noisy, target = mix(rows, sample)
        output = chip_sum[0, here].astype(jnp.float32)
        for p in range(1, nx):
            output = output + chip_sum[p, here].astype(jnp.float32)
        gate = modulation_ref[pl.ds(sample, 1), 2 * features :]
        errors = noisy + gate * output - target
        weight = weight_ref[sample]
        slopes[rows] = (scale_all * weight * gate * errors).astype(jnp.bfloat16)
        return total + weight * jnp.sum(errors * errors, -1, keepdims=True)

    squares = lax.fori_loop(0, half // CHUNK, slope_step, jnp.zeros((CHUNK, 1), jnp.float32))
    own_slopes = slopes.at[own_rows]
    slopes_copy = remote(own_slopes, own_slopes, slopes_sem.at[0], slopes_sem.at[1], mate)
    slopes_copy.start()
    loss_part = jnp.sum(squares) / (rows_per * features)
    core_tile[core] = jnp.full((8, LANES), loss_part, jnp.float32)
    core_copy = remote(
        core_tile.at[core], core_tile.at[core], core_sem.at[0], core_sem.at[1], mate
    )
    core_copy.start()
    slopes_copy.wait_recv()

    slope_all = lax.dot_general(
        down[...], slopes[...], (((1,), (1,)), ((), ())), preferred_element_type=jnp.float32
    )
    for d in range(ndp):
        part = slice(d * share, (d + 1) * share)
        pre_out[d] = (slope_all[part] * slope_t[part, :]).astype(jnp.bfloat16)
    pre_in[me] = pre_out[me]
    pre_copies = [
        remote(pre_out.at[peer[0]], pre_in.at[me], pre_send.at[peer[0]], pre_recv.at[me], peer)
        for peer in others
    ]
    for copy in pre_copies:
        copy.start()

    core_copy.wait_recv()
    weight_here = weight_ref[0]
    for sample in range(1, samples):
        weight_here = weight_here + weight_ref[sample]
    line = lax.broadcasted_iota(jnp.int32, (8, LANES), 0)
    all_tile[me] = jnp.where(line == 0, core_tile[0] + core_tile[1], weight_here)
    tile_copies = [
        remote(all_tile.at[me], all_tile.at[me], tile_send.at[peer[0]], tile_recv.at[me], peer)
        for peer in others
    ]
    for copy in tile_copies:
        copy.start()

    walk_y(0, share_y)
    for k in range(2, nz):
        walk_z(k, relay)
        walk_y(k - 1, share_y)
        walk_y(k - 2, share_x)
    if nz > 1:
        walk_y(nz - 1, share_y)
        walk_y(nz - 2, share_x)
    walk_y(nz - 1, share_x)

    grad_ref[...] = jnp.dot(pre_in[me], rows_all[me], preferred_element_type=jnp.float32)

    def grad_step(k, carry):
        block = lax.rem(me + k, ndp)

        @pl.when(lax.rem(block, ny) == y)
        def own_column():
            await_own_column(block)

        @pl.when(lax.rem(block, ny) != y)
        def other_column():
            await_other_column(block)

        remote(
            pre_out.at[block], pre_in.at[block], pre_send.at[block], pre_recv.at[block], mate
        ).wait_recv()
        grad_ref[...] += jnp.dot(
            pre_in[block], rows_all[block], preferred_element_type=jnp.float32
        )
        return carry

    lax.fori_loop(1, ndp, grad_step, 0)

    for peer in others:
        block = peer[0]
        remote(
            all_tile.at[block], all_tile.at[block], tile_send.at[block], tile_recv.at[block], peer
        ).wait_recv()
    sums = all_tile[0]
    for d in range(1, ndp):
        sums = sums + all_tile[d]
    loss_sum, weight_sum = sums[0, 0], sums[1, 0]
    grad_ref[...] = grad_ref[...] / weight_sum
    sums_ref[0, 0] = loss_sum / weight_sum

    @pl.when(z > 0)
    def first_down_sent():
        to_z(me, 0).wait_send()

    @pl.when(z < nz - 1)
    def first_up_sent():
        to_z(me, 1).wait_send()

    for copy in to_y(me) + [part_copy, slopes_copy, core_copy]:
        copy.wait_send()
    for copy in chip_copies + pre_copies + tile_copies:
        copy.wait_send()
    for k in range(1, nz):
        walk_z(k, drain)
    for k in range(nz):
        walk_y(k, drain_y)


def local_kernel(sizes, clean, noise, modulation, strata, up_weight, down_weight):
    samples_here, rows_per, features = clean.shape
    nz, ny, nx = sizes
    ndp, tokens, units = nz * ny, samples_here * rows_per, up_weight.shape[1]
    half, share, padded = tokens // CORES, units // ndp, pl.cdiv(units, LANES) * LANES
    fraction, weight = stratum_weights(strata)
    bf16, f32 = jnp.bfloat16, jnp.float32
    vmem = pl.BlockSpec(memory_space=pltpu.VMEM)
    smem = pl.BlockSpec(memory_space=pltpu.SMEM)
    anywhere = pl.BlockSpec(memory_space=pl.ANY)
    dma = pltpu.SemaphoreType.DMA
    gradient, loss = pl.pallas_call(
        functools.partial(step_kernel, (nz, ny, nx, rows_per)),
        out_shape=(
            jax.ShapeDtypeStruct((share, features), f32),
            jax.ShapeDtypeStruct((1, 1), f32),
        ),
        in_specs=[smem, smem, vmem, vmem, vmem, anywhere, anywhere],
        out_specs=(vmem, smem),
        scratch_shapes=[
            pltpu.VMEM((units, features), bf16),
            pltpu.VMEM((units, features), bf16),
            pltpu.VMEM((ndp, tokens, features), bf16),
            pltpu.VMEM((padded, tokens), f32),
            pltpu.VMEM((padded, tokens), f32),
            pltpu.VMEM((tokens, padded), bf16),
            pltpu.VMEM((half, features), bf16),
            pltpu.VMEM((half, features), bf16),
            pltpu.VMEM((half, features), f32),
            pltpu.VMEM((nx, half, features), bf16),
            pltpu.VMEM((tokens, features), bf16),
            pltpu.VMEM((ndp, share, tokens), bf16),
            pltpu.VMEM((ndp, share, tokens), bf16),
            pltpu.VMEM((CORES, 8, LANES), f32),
            pltpu.VMEM((ndp, 8, LANES), f32),
            dma((2,)),
            dma((ndp * (CORES * nx + ny + nx),)),
            dma((ndp * CORES * nx,)),
            dma((2,)),
            dma((nx,)),
            dma((nx,)),
            dma((2,)),
            dma((2,)),
            dma((ndp,)),
            dma((ndp,)),
            dma((ndp,)),
            dma((ndp,)),
        ],
        compiler_params=pltpu.CompilerParams(
            collective_id=0, has_side_effects=True, vmem_limit_bytes=60 * 1024 * 1024
        ),
    )(
        fraction,
        weight,
        clean.reshape(tokens, features),
        noise.reshape(tokens, features),
        modulation,
        up_weight.T,
        down_weight,
    )
    return (gradient, loss.reshape(()))


def chip_sizes(mesh):
    if mesh.shape["mp"] % CORES:
        return None
    spots = [tuple(d.coords) for d in mesh.devices[:, 0]]
    ny = len({spot[1] for spot in spots})
    return (mesh.shape["dp"] // ny, ny, mesh.shape["mp"] // CORES)


def local(sizes, clean, *others):
    gathered = lax.axis_size("dp") * clean.size * clean.dtype.itemsize
    units = others[-1].shape[0]
    half = clean.shape[0] * clean.shape[1] // CORES
    if gathered > GATHER_LIMIT_BYTES:
        return local_scatter(clean, *others)
    if units % (8 * lax.axis_size("dp")) or half % (LANES // 2 * (lax.axis_size("mp") // CORES)) or clean.shape[1] % CHUNK:
        return local_gather(clean, *others)
    return local_kernel(sizes, clean, *others)


def solution(mesh):
    return jax.shard_map(
        functools.partial(local, chip_sizes(mesh)),
        mesh=mesh,
        in_specs=(
            P("dp", None, None),
            P("dp", None, None),
            P("dp", None),
            P("dp"),
            P(None, "mp"),
            P("mp", None),
        ),
        out_specs=(P(("mp", "dp"), None), P()),
        check_vma=False,
    )
```
